256 devices in a mesh: dp: 16 (over z, core), tensor: 16 (over y, x).
Axes of the slice: x: 4, y: 4, z: 8, core: 2. Of those that a mesh axis runs over, the one named last changes fastest.
Arguments:
- tokens: bfloat16 [8192, 4096], P(('dp', 'tensor')), parts along dimension 0, may hold values from -6 to 6
- norm_gain: float32 [4096], replicated, may hold values from 0.1 to 1.9
- gate_w: bfloat16 [4096, 2048], P(None, 'tensor'), may hold values from -0.09375 to 0.09375
- up_w: bfloat16 [4096, 2048], P(None, 'tensor'), may hold values from -0.09375 to 0.09375
- down_w: bfloat16 [2048, 4096], P('tensor'), may hold values from -0.125 to 0.125
- final_gain: float32 [4096], replicated, may hold values from 0.1 to 1.9
- vocab_w: bfloat16 [18432, 4096], P('tensor')
- targets: int32 [8192], P(('dp', 'tensor')), parts along dimension 0, may hold values from 0 to 18431
- lengths: int32 [64], P('dp'), parts along dimension 0, may hold values from 1 to 128
Outputs:
- losses: float32 [8192], P(('dp', 'tensor')), parts along dimension 0
The draws below stay inside these ranges and needn't reach their ends.
There are 16 independent parts, one for each index of `dp`. The reference program is written for one: setup_inputs(seed, part) draws one part's arguments, and reference() takes and returns one part's arrays. A program takes and returns all parts, laid end to end along the dimension named above; an argument that names none is the same for every part. Nothing has to cross between parts.
All inputs are finite; a program needn't handle non-finite values.
Results may differ from the reference program's by a relative error of at most 0.014.
Values may be sent and summed in bfloat16 or wider, within the bound.
No kernel may reach another device: no remote copies, remote signals or barrier semaphores. Data moves between devices by JAX's collectives and lax.ppermute only.
A program may use at most 64 MiB of HBM per device.

```python
import math
import jax
import jax.numpy as jnp
from jax import lax

D = 4096
FF_DEV = 128
PACK_LEN = 128
TOKENS = 512
PACKS = 4
FF = 2048
VOCAB = 18432
N_TENSOR = 16


def draw_vocab_w(key, part):
    key_base = jax.random.fold_in(jax.random.fold_in(key, 17), 0)
    weights = jax.random.normal(key_base, (VOCAB, D), jnp.float32) * (3.0 / math.sqrt(D))
    return weights.astype(jnp.bfloat16)


def place_ends(entries, key, least, high):
    longest = entries.shape.index(max(entries.shape))
    spots = []
    for shift in (0, 1):
        where = [jax.random.randint(jax.random.fold_in(key, axis), (), 0, length) for axis, length in enumerate(entries.shape)]
        where[longest] = (where[longest] + shift) % entries.shape[longest]
        spots.append(tuple(where))
    return entries.at[spots[0]].set(least).at[spots[1]].set(high)


def levels(rng, dims, pieces, least, largest):
    gain, own = 1.0, jax.random.fold_in(rng, 6)
    for axis_at, parts in pieces:
        heights = jnp.exp(jax.random.uniform(jax.random.fold_in(own, axis_at), (parts,), jnp.float32, least / len(pieces), largest / len(pieces)))
        gain = gain * jnp.repeat(heights, dims[axis_at] // parts).reshape([-1 if axis == axis_at else 1 for axis in range(len(dims))])
    return gain


def bell_draw(stream_key, dims, spread, limit, cuts=(), kind=jnp.bfloat16):
    entries = jax.random.normal(stream_key, dims, jnp.float32) * spread
    if len(cuts) > 0:
        entries = levels(stream_key, dims, cuts, -0.22, 0.18) * entries
    return jnp.clip(entries, min=-limit, max=limit).astype(kind)


def setup_inputs(seed: int = 0, part: int = 0) -> dict:
    arg_keys = jax.random.split(jax.random.key(seed), 10)
    part_splits = jax.random.split(jax.random.fold_in(arg_keys[9], part), 10)
    tokens = bell_draw(part_splits[0], (TOKENS, D), 1.0, 6.0, ((0, 16),))
    norm_gain = jnp.clip(1.0 + 0.18 * jax.random.normal(arg_keys[1], (D,), jnp.float32), 0.1, 1.9)
    gate_w = bell_draw(arg_keys[2], (D, FF), D ** -0.5, 0.09375, ((1, 16),))
    up_w = bell_draw(arg_keys[3], (D, FF), D ** -0.5, 0.09375, ((1, 16),))
    down_w = bell_draw(arg_keys[4], (FF, D), FF ** -0.5, 0.125, ((0, 16),))
    final_gain = jnp.clip(1.0 + 0.18 * jax.random.normal(arg_keys[5], (D,), jnp.float32), 0.1, 1.9)
    vocab_w = draw_vocab_w(jax.random.fold_in(arg_keys[9], 71), part)
    targets = place_ends(jax.random.randint(part_splits[7], (TOKENS,), 0, VOCAB), jax.random.fold_in(part_splits[7], 1), 0, VOCAB - 1).astype(jnp.int32)
    lengths = place_ends(jax.random.randint(part_splits[8], (PACKS,), 1, PACK_LEN + 1), jax.random.fold_in(part_splits[8], 1), 1, PACK_LEN).astype(jnp.int32)
    return {"tokens": tokens, "norm_gain": norm_gain, "gate_w": gate_w, "up_w": up_w, "down_w": down_w, "final_gain": final_gain, "vocab_w": vocab_w, "targets": targets, "lengths": lengths}


def scaled_norm(values, scale_gain):
    widened = values.astype(jnp.float32)
    return widened * lax.rsqrt(lax.optimization_barrier(jnp.mean(widened * widened, axis=1, keepdims=True)) + 1e-06) * scale_gain

def reference(tokens, norm_gain, gate_w, up_w, down_w, final_gain, vocab_w, targets, lengths):
    normed = scaled_norm(tokens, norm_gain).astype(jnp.bfloat16)
    gate_vals = jnp.dot(normed, gate_w, preferred_element_type=jnp.float32)
    up_vals = jnp.dot(normed, up_w, preferred_element_type=jnp.float32)
    hidden = (jax.nn.silu(gate_vals) * up_vals).astype(jnp.bfloat16)

    def add_block(block_index, running):
        begin = jnp.asarray(block_index * FF_DEV).astype(jnp.int32)
        hidden_part = lax.dynamic_slice_in_dim(hidden, begin, FF_DEV, 1)
        weight_part = lax.dynamic_slice_in_dim(down_w, begin, FF_DEV, 0)
        term = jnp.dot(hidden_part, weight_part, preferred_element_type=jnp.float32).astype(jnp.bfloat16)
        term = lax.optimization_barrier(term)
        return running + term.astype(jnp.float32)
    branch_sum = lax.fori_loop(0, N_TENSOR, add_block, jnp.zeros((TOKENS, D), jnp.float32))
    summed = (tokens.astype(jnp.float32) + branch_sum).astype(jnp.bfloat16)
    final_rows = scaled_norm(summed, final_gain).astype(jnp.bfloat16)
    logits = jnp.dot(final_rows, vocab_w.T, preferred_element_type=jnp.float32)
    row_max = lax.optimization_barrier(jnp.max(logits, axis=1))
    log_total = row_max + jnp.log(lax.optimization_barrier(jnp.sum(jnp.exp(logits - row_max[:, None]), axis=1)))
    target_logit = jnp.take_along_axis(logits, targets[:, None].astype(jnp.int32), axis=1)[:, 0]
    positions = jnp.arange(TOKENS, dtype=jnp.int32)
    pack_ids = (positions // PACK_LEN).astype(jnp.int32)
    limits = lengths[pack_ids]
    valid = positions % PACK_LEN < limits
    return jnp.where(valid, log_total - target_logit, jnp.float32(0.0))
```

```python
import jax
import jax.numpy as jnp
from jax import lax
from jax.experimental import pallas as pl
from jax.experimental.pallas import tpu as pltpu
from jax.sharding import PartitionSpec as P

PACK_LEN = 128
SIDE = 4
OFFSETS = (0, SIDE - 1, 1, 2)
EPS = 1e-06


def shifted(values, axis, step):
    pairs = []
    for y in range(SIDE):
        for x in range(SIDE):
            to_y, to_x = ((y + step) % SIDE, x) if axis == "y" else (y, (x + step) % SIDE)
            pairs.append((y * SIDE + x, to_y * SIDE + to_x))
    return lax.ppermute(values, "tensor", pairs)


def ring_stack(values, axis):
    half = values.shape[-2] // 2
    lower, upper = shifted(values, axis, 1), shifted(values, axis, -1)
    top = shifted(lower[..., :half, :], axis, 1)
    bottom = shifted(upper[..., half:, :], axis, -1)
    return jnp.stack([values, lower, upper, jnp.concatenate([top, bottom], -2)], 0)


def gathered(first, second):
    first_row, second_row = ring_stack(first, "x"), ring_stack(second, "y")
    return ring_stack(first_row, "y"), ring_stack(second_row, "x")


def place(base, offset):
    return lax.rem(base + OFFSETS[offset], SIDE)


VMEM = pl.BlockSpec(memory_space=pltpu.VMEM)
SMEM = pl.BlockSpec(memory_space=pltpu.SMEM)


def up_kernel(at, first, second, gain, gate_w, up_w, hidden, kept, extra, sums, squares):
    rows, width = first.shape[2], second.shape[3]
    tokens, step = SIDE * SIDE * rows, 512
    for side, ref in enumerate((first, second)):
        for k in range(0, width, step):
            row = side * width + k
            values = ref[:, :, :, k : k + step].reshape(tokens, step).astype(jnp.float32)
            wide = values * values
            part = wide[:, :128]
            for c in range(128, step, 128):
                part += wide[:, c : c + 128]
            scaled = (values * gain[:, row : row + step]).astype(jnp.bfloat16)
            weights = jnp.concatenate([gate_w[row : row + step], up_w[row : row + step]], axis=1)
            product = jnp.dot(scaled, weights, preferred_element_type=jnp.float32)
            if k == 0:
                sums[side], squares[side] = product, part
            else:
                sums[side] += product
                squares[side] += part
    y, x = at[0], at[1]
    mine = y * SIDE + x
    column = pl.multiple_of(lax.rem(mine, SIDE * SIDE // 2) * 256, 256)
    for dy in range(SIDE):
        for dx in range(SIDE):
            i, j = (dy * SIDE + dx) * rows, (dx * SIDE + dy) * rows
            spot = place(y, dy) * SIDE + place(x, dx)
            total = squares[0, i : i + rows] + squares[1, j : j + rows]
            scale = lax.rsqrt(jnp.sum(total, axis=1, keepdims=True) / (2 * width) + EPS)
            both = (sums[0, i : i + rows] + sums[1, j : j + rows]) * scale
            gate, up = both[:, :128], both[:, 128:]
            hidden[spot] = (gate / (1.0 + jnp.exp(-gate)) * up).astype(jnp.bfloat16)
            kept[spot] = jnp.where(
                mine < SIDE * SIDE // 2,
                first[dy, dx, :, pl.ds(column, 256)],
                second[dx, dy, :, pl.ds(column, 256)],
            )
            extra[spot] = first[dy, dx, :16, width : width + 128]


def down_kernel(at, first, second, weights, kept, out_first, out_second):
    y, x = at[0], at[1]
    rows = first.shape[2]
    for side, (ref, out) in enumerate(((first, out_first), (second, out_second))):
        total = kept[side * rows : (side + 1) * rows].astype(jnp.float32)
        for dy in range(SIDE):
            for dx in range(0, SIDE, 2):
                pair = [ref[dy, d] if side == 0 else ref[d, dy] for d in (dx, dx + 1)]
                rhs = [weights[place(y, dy) * SIDE + place(x, d)] for d in (dx, dx + 1)]
                total += jnp.dot(
                    jnp.concatenate(pair, axis=1),
                    jnp.concatenate(rhs, axis=0),
                    preferred_element_type=jnp.float32,
                )
        out[...] = total.astype(jnp.bfloat16)


def vocab_kernel(at, first, second, gain, vocab_w, targets, out, logits, squares):
    step = pl.program_id(0)
    rows = first.shape[2]
    dy, dx = step // SIDE, lax.rem(step, SIDE)

    @pl.when(step == 0)
    def _():
        logits[...] = jnp.zeros_like(logits)
        squares[...] = jnp.zeros_like(squares)

    for side in range(2):
        values = (first[dy, dx] if side == 0 else second[dx, dy]).astype(jnp.float32)
        here = slice(side * rows, (side + 1) * rows)
        wide = values * values
        squares[here] += wide[:, :128] + wide[:, 128:]
        scaled = (values * gain[0]).astype(jnp.bfloat16)
        logits[:, here] += lax.dot_general(
            vocab_w[...], scaled, (((1,), (1,)), ((), ())), preferred_element_type=jnp.float32
        )

    @pl.when(step == SIDE * SIDE - 1)
    def _():
        vocab = logits.shape[0]
        width = 256 * SIDE * SIDE
        total = jnp.sum(squares[...].T, axis=0, keepdims=True)
        values = logits[...] * lax.rsqrt(total / width + EPS)
        largest = jnp.max(values, axis=0, keepdims=True)
        out[0:1] = largest
        out[1:2] = jnp.sum(jnp.exp(values - largest), axis=0, keepdims=True)
        wanted = targets[...] - (at[0] * SIDE + at[1]) * vocab
        found = lax.broadcasted_iota(jnp.int32, values.shape, 0) == wanted
        out[2:3] = jnp.sum(jnp.where(found, values, 0.0), axis=0, keepdims=True)


def block_at(step, at):
    offsets = lambda i: jnp.where(i == 1, SIDE - 1, jnp.where(i == 2, 1, jnp.where(i == 3, 2, 0)))
    y = lax.rem(at[0] + offsets(step // SIDE), SIDE)
    x = lax.rem(at[1] + offsets(lax.rem(step, SIDE)), SIDE)
    return y * SIDE + x


def body(tokens, norm_gain, gate_w, up_w, down_w, final_gain, vocab_w, targets, lengths):
    tok_local, width = tokens.shape
    peers = SIDE * SIDE
    count, half = peers * tok_local, width // 2
    hidden_dev, slice_w = gate_w.shape[1], width // peers
    mine = lax.axis_index("tensor")
    at = jnp.stack([mine // SIDE, lax.rem(mine, SIDE)]).astype(jnp.int32)

    digits = jnp.concatenate([targets // 256, targets % 256]).astype(jnp.bfloat16)
    digits = jnp.pad(digits[None], ((0, tok_local - 1), (0, 128 - 2 * tok_local)))
    first, second = gathered(
        jnp.concatenate([tokens[:, :half], digits], axis=1), tokens[:, half:]
    )
    down_cols = lax.all_to_all(
        jnp.moveaxis(down_w.reshape(hidden_dev, peers, slice_w), 1, 0), "tensor", 0, 0, tiled=True
    )

    bf16, f32 = jnp.bfloat16, jnp.float32
    hidden, kept, extra = pl.pallas_call(
        up_kernel,
        out_shape=(
            jax.ShapeDtypeStruct((peers, tok_local, hidden_dev), bf16),
            jax.ShapeDtypeStruct((peers, tok_local, slice_w), bf16),
            jax.ShapeDtypeStruct((peers, 16, 128), bf16),
        ),
        in_specs=[SMEM] + [VMEM] * 5,
        out_specs=(VMEM,) * 3,
        scratch_shapes=[
            pltpu.VMEM((2, count, 2 * hidden_dev), f32),
            pltpu.VMEM((2, count, 128), f32),
        ],
        cost_estimate=pl.CostEstimate(
            flops=4 * count * width * hidden_dev, transcendentals=0, bytes_accessed=8 << 20
        ),
    )(at, first, second, norm_gain[None], gate_w, up_w)

    hidden = hidden.reshape(count, hidden_dev)
    first, second = gathered(hidden[: count // 2], hidden[count // 2 :])
    out_half = jax.ShapeDtypeStruct((count // 2, slice_w), bf16)
    first, second = pl.pallas_call(
        down_kernel,
        out_shape=(out_half, out_half),
        in_specs=[SMEM] + [VMEM] * 4,
        out_specs=(VMEM, VMEM),
        cost_estimate=pl.CostEstimate(
            flops=2 * count * width * hidden_dev, transcendentals=0, bytes_accessed=4 << 20
        ),
    )(at, first, second, down_cols, kept.reshape(count, slice_w))
    first, second = gathered(first, second)

    high, low = extra[:, 0, :tok_local], extra[:, 0, tok_local : 2 * tok_local]
    all_targets = high.astype(jnp.int32) * 256 + low.astype(jnp.int32)
    vocab = vocab_w.shape[0]
    stats = pl.pallas_call(
        vocab_kernel,
        out_shape=jax.ShapeDtypeStruct((8, count), f32),
        grid_spec=pltpu.PrefetchScalarGridSpec(
            num_scalar_prefetch=1,
            grid=(peers,),
            in_specs=[
                VMEM,
                VMEM,
                pl.BlockSpec((1, 1, slice_w), lambda i, at: (block_at(i, at), 0, 0)),
                pl.BlockSpec((vocab, slice_w), lambda i, at: (0, block_at(i, at))),
                VMEM,
            ],
            out_specs=pl.BlockSpec((8, count), lambda i, at: (0, 0)),
            scratch_shapes=[pltpu.VMEM((vocab, count), f32), pltpu.VMEM((count, 128), f32)],
        ),
        cost_estimate=pl.CostEstimate(
            flops=2 * count * width * vocab, transcendentals=count * vocab, bytes_accessed=14 << 20
        ),
    )(at, first, second, final_gain.reshape(peers, 1, slice_w), vocab_w, all_targets.reshape(1, count))

    stats = jnp.moveaxis(stats[:3].reshape(3, peers, tok_local), 1, 0)
    stats = lax.all_to_all(stats, "tensor", 0, 0, tiled=True)
    largest = jnp.max(stats[:, 0], axis=0)
    total = jnp.sum(stats[:, 1] * jnp.exp(stats[:, 0] - largest), axis=0)
    own_losses = largest + jnp.log(total) - jnp.sum(stats[:, 2], axis=0)
    positions = mine * tok_local + lax.broadcasted_iota(jnp.int32, (tok_local,), 0)
    pack_ids = positions // PACK_LEN
    matches = pack_ids[:, None] == lax.broadcasted_iota(jnp.int32, (1, lengths.shape[0]), 1)
    limits = jnp.sum(jnp.where(matches, lengths[None, :], 0), axis=1)
    return jnp.where(positions % PACK_LEN < limits, own_losses, jnp.float32(0.0))


def solution(mesh):
    return jax.shard_map(
        body,
        mesh=mesh,
        in_specs=(
            P(("dp", "tensor"), None),
            P(),
            P(None, "tensor"),
            P(None, "tensor"),
            P("tensor", None),
            P(),
            P("tensor", None),
            P(("dp", "tensor")),
            P("dp"),
        ),
        out_specs=P(("dp", "tensor")),
        check_vma=False,
    )
```

```python
import functools

import jax
import jax.numpy as jnp
from jax import lax
from jax.experimental import pallas as pl
from jax.experimental.pallas import tpu as pltpu
from jax.sharding import PartitionSpec as P

PACK_LEN = 128
SIDE = 4
OFFSETS = (0, SIDE - 1, 1, 2)
EPS = 1e-06
BF16, F32 = jnp.bfloat16, jnp.float32
VMEM = pl.BlockSpec(memory_space=pltpu.VMEM)
SMEM = pl.BlockSpec(memory_space=pltpu.SMEM)


def shifted(values, axis, step):
    pairs = []
    for y in range(SIDE):
        for x in range(SIDE):
            to_y, to_x = ((y + step) % SIDE, x) if axis == "y" else (y, (x + step) % SIDE)
            pairs.append((y * SIDE + x, to_y * SIDE + to_x))
    return lax.ppermute(values, "tensor", pairs)


def fanned(values, axis):
    return [values, shifted(values, axis, 1), shifted(values, axis, -1), shifted(values, axis, 2)]


def stack_kernel(at, *refs):
    for side, out in enumerate(refs[2 * SIDE :]):
        for block in range(SIDE):
            out[block] = refs[side * SIDE + block][...]


def gathered(at, first, second):
    inputs = (at, *fanned(first, "x"), *fanned(second, "y"))
    stacks = tuple(pltpu.VMEM((SIDE, *half.shape), half.dtype) for half in (first, second))
    first, second = call(stack_kernel, stacks, inputs, 1 << 16)
    return list(zip(fanned(first, "y"), fanned(second, "x")))


def place(base, offset):
    if not isinstance(offset, int):
        offset = jnp.where(offset == 1, SIDE - 1, jnp.where(offset == 0, 0, offset - 1))
    else:
        offset = OFFSETS[offset]
    return lax.rem(base + offset, SIDE)


def call(kernel, out_shape, inputs, flops, scratch=()):
    inputs = inputs[:1] + tuple(pltpu.with_memory_space_constraint(a, pltpu.VMEM) for a in inputs[1:])
    return pl.pallas_call(
        kernel,
        compiler_params=pltpu.CompilerParams(vmem_limit_bytes=24 << 20),
        out_shape=out_shape,
        in_specs=[SMEM] + [VMEM] * (len(inputs) - 1),
        out_specs=jax.tree.map(lambda _: VMEM, out_shape),
        scratch_shapes=list(scratch),
        cost_estimate=pl.CostEstimate(flops=flops, transcendentals=0, bytes_accessed=1 << 20),
    )(*inputs)


def up_part(at, *refs, groups):
    pieces, (gain, gate_w, up_w, sums, squares, kept, extra) = refs[: 2 * groups], refs[2 * groups :]
    blocks, rows, width = pieces[1].shape
    tokens, step = blocks * rows, 512
    for side in range(2):
        for k in range(0, width, step):
            row = side * width + k
            values = [ref[:, :, k : k + step].reshape(tokens, step) for ref in pieces[side::2]]
            values = jnp.concatenate(values, axis=0).astype(F32)
            wide = values * values
            part = wide[:, :128]
            for c in range(128, step, 128):
                part += wide[:, c : c + 128]
            scaled = (values * gain[:, row : row + step]).astype(BF16)
            weights = jnp.concatenate([gate_w[row : row + step], up_w[row : row + step]], axis=1)
            product = jnp.dot(scaled, weights, preferred_element_type=F32)
            product = product.reshape(groups, blocks, rows, product.shape[1])
            part = part.reshape(groups, blocks, rows, 128)
            if k == 0:
                sums[:, side], squares[:, side] = product, part
            else:
                sums[:, side] += product
                squares[:, side] += part
    mine, peers = at[0] * SIDE + at[1], SIDE * SIDE
    slice_w = 2 * width // peers
    column = pl.multiple_of(lax.rem(mine, peers // 2) * slice_w, slice_w)
    for group in range(groups):
        first, second = pieces[2 * group : 2 * group + 2]
        here = pl.ds(column, slice_w)
        kept[group] = jnp.where(mine < peers // 2, first[:, :, here], second[:, :, here])
        extra[group] = first[:, :16, width : width + 128]


def up_end(at, *refs, width):
    parts, (hidden, kept, extra) = [refs[4 * i : 4 * i + 4] for i in range(3)], refs[12:]
    where = ((0, 0), (1, 0), (1, 1), (2, 0))
    y, x = at[0], at[1]
    low = y * SIDE + x < SIDE * SIDE // 2
    for dy in range(SIDE):
        for dx in range(SIDE):
            (part_a, a), (part_b, b) = where[dy], where[dx]
            spot = place(y, dy) * SIDE + place(x, dx)
            total = parts[part_a][1][a, 0, dx] + parts[part_b][1][b, 1, dy]
            scale = lax.rsqrt(jnp.sum(total, axis=1, keepdims=True) / width + EPS)
            both = (parts[part_a][0][a, 0, dx] + parts[part_b][0][b, 1, dy]) * scale
            gate, up = both[:, :128], both[:, 128:]
            hidden[spot] = (gate / (1.0 + jnp.exp(-gate)) * up).astype(BF16)
            kept[spot] = jnp.where(low, parts[part_a][2][a, dx], parts[part_b][2][b, dy])
            extra[spot] = parts[part_a][3][a, dx]


def down_kernel(at, *refs):
    pieces, (weights, kept, out_first, out_second) = refs[:8], refs[8:]
    y, x = at[0], at[1]
    rows = pieces[0].shape[1]
    for side, out in enumerate((out_first, out_second)):
        total = kept[side * rows : (side + 1) * rows].astype(F32)
        for group in range(SIDE):
            for block in range(0, SIDE, 2):
                lhs, rhs = [], []
                for b in (block, block + 1):
                    dy, dx = (group, b) if side == 0 else (b, group)
                    lhs.append(pieces[2 * group + side][b])
                    rhs.append(weights[place(y, dy) * SIDE + place(x, dx)])
                total += jnp.dot(
                    jnp.concatenate(lhs, axis=1), jnp.concatenate(rhs, axis=0), preferred_element_type=F32
                )
        out[...] = total.astype(BF16)


def vocab_part(at, *refs, groups, last):
    pieces, refs = refs[: 2 * len(groups)], refs[2 * len(groups) :]
    gain, vocab_w, refs = refs[0], refs[1], refs[2:]
    begin = groups[0] == 0
    before, refs = (None, refs) if begin else (refs[:2], refs[2:])
    targets, refs = (refs[0], refs[1:]) if last else (None, refs)
    out = refs[0] if last else None
    logits, squares = refs[1:] if last else refs
    slice_w = gain.shape[2]
    for side in range(2):
        rows = pieces[side].shape[1]
        here = slice(side * rows, (side + 1) * rows)
        total, square = None, None
        for number, group in enumerate(groups):
            for block in range(SIDE):
                dy, dx = (group, block) if side == 0 else (block, group)
                spot = place(at[0], dy) * SIDE + place(at[1], dx)
                values = pieces[2 * number + side][block].astype(F32)
                wide = values * values
                wide = wide[:, :128] + wide[:, 128:]
                scaled = (values * gain[spot]).astype(BF16)
                term = lax.dot_general(
                    vocab_w[:, pl.ds(pl.multiple_of(spot * slice_w, slice_w), slice_w)],
                    scaled,
                    (((1,), (1,)), ((), ())),
                    preferred_element_type=F32,
                )
                if number == 0 and block == 0:
                    if begin:
                        logits[:, here], squares[here] = term, wide
                    else:
                        logits[:, here] = before[0][:, here] + term
                        squares[here] = before[1][here] + wide
                else:
                    logits[:, here] += term
                    squares[here] += wide
    if last:
        vocab, width = vocab_w.shape
        total = jnp.sum(squares[...].T, axis=0, keepdims=True)
        values = logits[...] * lax.rsqrt(total / width + EPS)
        largest = jnp.max(values, axis=0, keepdims=True)
        out[0:1] = largest
        out[1:2] = jnp.sum(jnp.exp(values - largest), axis=0, keepdims=True)
        wanted = targets[...] - (at[0] * SIDE + at[1]) * vocab
        found = lax.broadcasted_iota(jnp.int32, values.shape, 0) == wanted
        out[2:3] = jnp.sum(jnp.where(found, values, 0.0), axis=0, keepdims=True)


def up_stage(at, groups, gain, gate_w, up_w, peers):
    blocks, rows, half = groups[0][1].shape
    width, hidden_dev = 2 * half, gate_w.shape[1]
    results = []
    for chosen in (groups[:1], groups[1:3], groups[3:]):
        n = len(chosen)
        out_shape = (
            pltpu.VMEM((n, 2, blocks, rows, 2 * hidden_dev), F32),
            pltpu.VMEM((n, 2, blocks, rows, 128), F32),
            pltpu.VMEM((n, blocks, rows, width // peers), BF16),
            pltpu.VMEM((n, blocks, 16, 128), BF16),
        )
        inputs = (at, *(piece for pair in chosen for piece in pair), gain, gate_w, up_w)
        flops = 4 * n * blocks * rows * width * hidden_dev
        results += call(functools.partial(up_part, groups=n), out_shape, inputs, flops)
    out_shape = (
        pltpu.VMEM((peers, rows, hidden_dev), BF16),
        pltpu.VMEM((peers, rows, width // peers), BF16),
        pltpu.VMEM((peers, 16, 128), BF16),
    )
    return call(functools.partial(up_end, width=width), out_shape, (at, *results), 1 << 20)


def vocab_stage(at, groups, gain, vocab_w, targets):
    vocab, width = vocab_w.shape
    count = targets.shape[1]
    sums = (pltpu.VMEM((vocab, count), F32), pltpu.VMEM((count, 128), F32))
    results = ()
    for chosen in ((0,), (1, 2), (3,)):
        last = chosen[-1] == SIDE - 1
        pieces = (piece for group in chosen for piece in groups[group])
        inputs = (at, *pieces, gain, vocab_w, *results) + ((targets,) if last else ())
        kernel = functools.partial(vocab_part, groups=chosen, last=last)
        flops = 2 * count * width * vocab * len(chosen) // SIDE
        if last:
            return call(kernel, pltpu.VMEM((8, count), F32), inputs, flops, sums)
        results = call(kernel, sums, inputs, flops)


def body(tokens, norm_gain, gate_w, up_w, down_w, final_gain, vocab_w, targets, lengths):
    tok_local, width = tokens.shape
    peers = SIDE * SIDE
    count, half = peers * tok_local, width // 2
    hidden_dev, slice_w = gate_w.shape[1], width // peers
    mine = lax.axis_index("tensor")
    at = jnp.stack([mine // SIDE, lax.rem(mine, SIDE)]).astype(jnp.int32)

    digits = jnp.concatenate([targets // 256, targets % 256]).astype(BF16)
    digits = jnp.pad(digits[None], ((0, tok_local - 1), (0, 128 - 2 * tok_local)))
    groups = gathered(at, jnp.concatenate([tokens[:, :half], digits], axis=1), tokens[:, half:])
    down_cols = lax.all_to_all(
        jnp.moveaxis(down_w.reshape(hidden_dev, peers, slice_w), 1, 0), "tensor", 0, 0, tiled=True
    )
    hidden, kept, extra = up_stage(at, groups, norm_gain[None], gate_w, up_w, peers)

    hidden = hidden.reshape(count, hidden_dev)
    groups = gathered(at, hidden[: count // 2], hidden[count // 2 :])
    out_half = pltpu.VMEM((count // 2, slice_w), BF16)
    inputs = (at, *(piece for pair in groups for piece in pair), down_cols, kept.reshape(count, slice_w))
    first, second = call(down_kernel, (out_half, out_half), inputs, 2 * count * width * hidden_dev)
    groups = gathered(at, first, second)

    high, low = extra[:, 0, :tok_local], extra[:, 0, tok_local : 2 * tok_local]
    all_targets = high.astype(jnp.int32) * 256 + low.astype(jnp.int32)
    stats = vocab_stage(
        at, groups, final_gain.reshape(peers, 1, slice_w), vocab_w, all_targets.reshape(1, count)
    )

    stats = jnp.moveaxis(stats[:3].reshape(3, peers, tok_local), 1, 0)
    stats = lax.all_to_all(stats, "tensor", 0, 0, tiled=True)
    largest = jnp.max(stats[:, 0], axis=0)
    total = jnp.sum(stats[:, 1] * jnp.exp(stats[:, 0] - largest), axis=0)
    own_losses = largest + jnp.log(total) - jnp.sum(stats[:, 2], axis=0)
    positions = mine * tok_local + lax.broadcasted_iota(jnp.int32, (tok_local,), 0)
    pack_ids = positions // PACK_LEN
    matches = pack_ids[:, None] == lax.broadcasted_iota(jnp.int32, (1, lengths.shape[0]), 1)
    limits = jnp.sum(jnp.where(matches, lengths[None, :], 0), axis=1)
    return jnp.where(positions % PACK_LEN < limits, own_losses, jnp.float32(0.0))


def solution(mesh):
    return jax.shard_map(
        body,
        mesh=mesh,
        in_specs=(
            P(("dp", "tensor"), None),
            P(),
            P(None, "tensor"),
            P(None, "tensor"),
            P("tensor", None),
            P(),
            P("tensor", None),
            P(("dp", "tensor")),
            P("dp"),
        ),
        out_specs=P(("dp", "tensor")),
        check_vma=False,
    )
```

```python
import functools

import jax
import jax.numpy as jnp
from jax import lax
from jax.experimental import pallas as pl
from jax.experimental.pallas import tpu as pltpu
from jax.sharding import PartitionSpec as P

PACK_LEN = 128
SIDE = 4
PEERS = SIDE * SIDE
OFFSETS = (0, SIDE - 1, 1, 2)
EXTRA = 16
EPS = 1e-06
BF16, F32 = jnp.bfloat16, jnp.float32
VMEM = pl.BlockSpec(memory_space=pltpu.VMEM)
SMEM = pl.BlockSpec(memory_space=pltpu.SMEM)
ANY = pl.BlockSpec(memory_space=pl.ANY)


def shifted(values, turn, step):
    pairs = []
    for part in range(lax.axis_size("dp")):
        for y in range(SIDE):
            for x in range(SIDE):
                along_x = (part % 2 == 0) == (turn == 0)
                to = (y, (x + step) % SIDE) if along_x else ((y + step) % SIDE, x)
                pairs.append((part * PEERS + y * SIDE + x, part * PEERS + to[0] * SIDE + to[1]))
    return lax.ppermute(values, ("dp", "tensor"), pairs)


def fanned(values):
    opposite = shifted(values, 0, 2)
    upper = shifted(values, 0, -1)
    return [values, shifted(values, 0, 1), upper, opposite]


def spot_of(at, group, block):
    ends = []
    for base, offset in ((at[0], group), (at[1], block)):
        ends.append(lax.rem(base + OFFSETS[offset], SIDE))
    return ends[0] * at[2] + ends[1] * at[3]


def call(kernel, out_shape, inputs, flops, scratch=()):
    inputs = inputs[:1] + tuple(pltpu.with_memory_space_constraint(a, pltpu.VMEM) for a in inputs[1:])
    return pl.pallas_call(
        kernel,
        compiler_params=pltpu.CompilerParams(vmem_limit_bytes=24 << 20),
        out_shape=out_shape,
        in_specs=[SMEM] + [VMEM] * (len(inputs) - 1),
        out_specs=jax.tree.map(lambda _: VMEM, out_shape),
        scratch_shapes=list(scratch),
        cost_estimate=pl.CostEstimate(flops=flops, transcendentals=0, bytes_accessed=1 << 20),
    )(*inputs)


def stack_kernel(at, *refs):
    for block in range(SIDE):
        refs[SIDE + block // 2][block % 2] = refs[block][...]


def gathered(at, values):
    half = pltpu.VMEM((2, *values.shape), values.dtype)
    low, high = call(stack_kernel, (half, half), (at, *fanned(values)), 1 << 16)
    lower_low, upper_high = shifted(low, 1, 1), shifted(high, 1, -1)
    lower_high, upper_low = shifted(high, 1, 1), shifted(low, 1, -1)
    far_low, far_high = shifted(lower_low, 1, 1), shifted(upper_high, 1, -1)
    return (
        ((0, 0, low), (0, 2, high)),
        ((1, 0, lower_low), (2, 2, upper_high), (1, 2, lower_high), (2, 0, upper_low)),
        ((3, 0, far_low), (3, 2, far_high)),
    )


def hold_vocab_kernel(at, after, source, out):
    pltpu.sync_copy(source, out)


def hold_up_kernel(at, gate_w, up_w, out, sems):
    width = gate_w.shape[1]
    copies = [
        pltpu.make_async_copy(ref, out.at[:, i * width : (i + 1) * width], sems.at[i])
        for i, ref in enumerate((gate_w, up_w))
    ]
    for copy in copies:
        copy.start()
    for copy in copies:
        copy.wait()


def held(kernel, out_shape, after, sources, scratch=()):
    after = tuple(pltpu.with_memory_space_constraint(a, pltpu.VMEM) for a in after)
    return pl.pallas_call(
        kernel,
        compiler_params=pltpu.CompilerParams(vmem_limit_bytes=1 << 20),
        out_shape=out_shape,
        in_specs=[SMEM] + [VMEM] * len(after) + [ANY] * (len(sources) - 1),
        out_specs=VMEM,
        scratch_shapes=list(scratch),
        cost_estimate=pl.CostEstimate(flops=1 << 31, transcendentals=0, bytes_accessed=16 << 20),
    )(sources[0], *after, *(pltpu.with_memory_space_constraint(a, pltpu.HBM) for a in sources[1:]))


def cut_kernel(at, weights, out):
    peers, rows, width = out.shape
    here = pl.ds(pl.multiple_of(at[4] * rows, rows), rows)
    for peer in range(peers):
        out[peer] = weights[here, peer * width : (peer + 1) * width]


def up_part(at, *refs, spots, earlier):
    count, last = len(spots), len(earlier) > 0
    pieces, (gain, weights), refs = refs[:count], refs[count : count + 2], refs[count + 2 :]
    sums, refs = refs[-1], refs[:-1]
    parts, ends = [], []
    if last:
        parts, ends, refs = [refs[0:2], refs[2:4]], refs[4:6], refs[6:]
    hidden, kept = refs
    blocks, rows, width = pieces[0].shape
    tokens, step = blocks * rows, 512
    square = None
    for k in range(0, width, step):
        values = [ref[:, :, k : k + step].reshape(tokens, step) for ref in pieces]
        values = jnp.concatenate(values, axis=0).astype(F32)
        wide = values * values
        for c in range(0, step, 128):
            part = wide[:, c : c + 128]
            square = part if square is None else square + part
        scaled = (values * gain[:, k : k + step]).astype(BF16)
        product = jnp.dot(scaled, weights[k : k + step], preferred_element_type=F32)
        if k == 0:
            sums[...] = product
        else:
            sums[...] += product
    both = sums[...] * lax.rsqrt(jnp.sum(square, axis=1, keepdims=True) / width + EPS)
    gate, up = both[:, : both.shape[1] // 2], both[:, both.shape[1] // 2 :]
    result = (gate / (1.0 + jnp.exp(-gate)) * up).astype(BF16)
    hidden[...] = result.reshape(hidden.shape)
    slice_w = width // PEERS
    here = pl.ds(pl.multiple_of(at[5] * slice_w, slice_w), slice_w)
    for number in range(count):
        kept[number] = pieces[number][:, :, here]
    if not last:
        return
    for places, part in zip((*earlier, spots), (*parts, (hidden, kept))):
        for number, (group, block) in enumerate(places):
            for b in range(blocks):
                spot = spot_of(at, group, block + b)
                for end, ref in zip(ends, part):
                    end[spot] = ref[number, b]


def down_kernel(at, *refs, spots):
    pieces, (own, partner, kept, digits, out) = refs[: len(spots)], refs[len(spots) :]
    low = at[4] == 0
    count = kept.shape[0]
    total = kept[...].astype(F32)
    for piece, (group, block) in zip(pieces, spots):
        rhs = []
        for b in range(2):
            spot = spot_of(at, group, block + b)
            rhs.append(jnp.where(low, own[spot], partner[spot]))
            rhs.append(jnp.where(low, partner[spot], own[spot]))
        lhs = jnp.concatenate([piece[0], piece[1]], axis=1)
        total += jnp.dot(lhs, jnp.concatenate(rhs, axis=0), preferred_element_type=F32)
    out[:count] = total.astype(BF16)
    out[count:] = digits[...]


def vocab_part(at, *refs, spots, begin, last):
    pieces, (gain, vocab_w), refs = refs[: len(spots)], refs[len(spots) : len(spots) + 2], refs[len(spots) + 2 :]
    before, refs = (None, refs) if begin else (refs[:3], refs[3:])
    out, refs = (refs[0], refs[1:]) if last else (None, refs)
    logits, squares, digits = refs
    slice_w, count = gain.shape[2], logits.shape[1]
    square, digit = None, None
    for number, piece in enumerate(pieces):
        for block in range(2):
            spot = spot_of(at, spots[number][0], spots[number][1] + block)
            values = piece[block, :count].astype(F32)
            wide = values * values
            wide = wide[:, :128] + wide[:, 128:]
            square = wide if square is None else square + wide
            extra = piece[block, count:].astype(F32)
            digit = extra if digit is None else digit + extra
            scaled = (values * gain[spot]).astype(BF16)
            term = lax.dot_general(
                vocab_w[:, pl.ds(pl.multiple_of(spot * slice_w, slice_w), slice_w)],
                scaled,
                (((1,), (1,)), ((), ())),
                preferred_element_type=F32,
            )
            if number == 0 and block == 0:
                logits[...] = term if begin else before[0][...] + term
            else:
                logits[...] += term
    if not begin:
        square, digit = square + before[1][...], digit + before[2][...]
    squares[...], digits[...] = square, digit
    if last:
        vocab, width = vocab_w.shape
        total = jnp.sum(square.T, axis=0, keepdims=True)
        values = logits[...] * lax.rsqrt(total / width + EPS)
        largest = jnp.max(values, axis=0, keepdims=True)
        out[0:1] = largest
        out[1:2] = jnp.sum(jnp.exp(values - largest), axis=0, keepdims=True)
        parts = count // slice_w
        high, low = (
            jnp.concatenate([digit[i * parts + p : i * parts + p + 1] for p in range(parts)], axis=1)
            for i in range(2)
        )
        wanted = (high * 256.0 + low).astype(jnp.int32) - at[5] * vocab
        found = lax.broadcasted_iota(jnp.int32, values.shape, 0) == wanted
        out[2:3] = jnp.sum(jnp.where(found, values, 0.0), axis=0, keepdims=True)


def split(pieces):
    return tuple(piece[:2] for piece in pieces), tuple(piece[2] for piece in pieces)


def up_stage(at, arrivals, gain, weights):
    blocks, rows, width = arrivals[0][0][2].shape
    both, slice_w = weights.shape[1], width // PEERS
    earlier, before = (), ()
    for arrived in arrivals:
        spots, pieces = split(arrived)
        n, last = len(pieces), arrived is arrivals[-1]
        part_shape = tuple(pltpu.VMEM((n, blocks, rows, w), BF16) for w in (both // 2, slice_w))
        end_shape = tuple(pltpu.VMEM((PEERS, rows, w), BF16) for w in (both // 2, slice_w))
        sums = pltpu.VMEM((n * blocks * rows, both), F32)
        inputs = (at, *pieces, gain, weights)
        flops = 2 * n * blocks * rows * width * both
        if last:
            kernel = functools.partial(up_part, spots=spots, earlier=earlier)
            return call(kernel, end_shape, inputs + before, flops, (*part_shape, sums))
        before += tuple(call(functools.partial(up_part, spots=spots, earlier=()), part_shape, inputs, flops, (sums,)))
        earlier += (spots,)


def vocab_stage(at, arrivals, gain, vocab_w, count):
    vocab, width = vocab_w.shape
    slice_w = width // PEERS
    sums = (
        pltpu.VMEM((vocab, count), F32),
        pltpu.VMEM((count, 128), F32),
        pltpu.VMEM((EXTRA, slice_w), F32),
    )
    results = ()
    for arrived in arrivals:
        spots, pieces = split(arrived)
        begin, last = arrived is arrivals[0], arrived is arrivals[-1]
        inputs = (at, *pieces, gain, vocab_w, *results)
        kernel = functools.partial(vocab_part, spots=spots, begin=begin, last=last)
        flops = 4 * count * width * vocab * len(pieces) // PEERS
        if last:
            return call(kernel, pltpu.VMEM((8, count), F32), inputs, flops, sums)
        results = call(kernel, sums, inputs, flops)


def body(tokens, norm_gain, gate_w, up_w, down_w, final_gain, vocab_w, targets, lengths):
    tok_local, width = tokens.shape
    count = PEERS * tok_local
    hidden_dev, slice_w = gate_w.shape[1], width // PEERS
    mine = lax.axis_index("tensor")
    core = lax.rem(lax.axis_index("dp"), 2)
    y, x = mine // SIDE, lax.rem(mine, SIDE)
    even = core == 0
    at = [jnp.where(even, y, x), jnp.where(even, x, y), jnp.where(even, SIDE, 1), jnp.where(even, 1, SIDE)]
    at = jnp.stack(at + [core, mine]).astype(jnp.int32)

    place = mine * tok_local + lax.broadcasted_iota(jnp.int32, (tok_local, 1), 0)
    found = place == lax.broadcasted_iota(jnp.int32, (tok_local, count), 1)
    digits = jnp.stack([targets // 256, targets % 256])[:, :, None]
    digits = jnp.sum(jnp.where(found[None], digits, 0), axis=1).astype(BF16).reshape(-1, slice_w)
    digits = jnp.pad(digits, ((0, EXTRA - digits.shape[0]), (0, 0)))

    arrivals = gathered(at, tokens)
    up_shape = pltpu.VMEM((width, 2 * hidden_dev), BF16)
    sems = pltpu.SemaphoreType.DMA((2,))
    weights = held(hold_up_kernel, up_shape, (), (at, gate_w, up_w), (sems,))

    down_half = call(cut_kernel, pltpu.VMEM((PEERS, hidden_dev // 2, slice_w), BF16), (at, down_w), 1 << 16)
    down_own = lax.all_to_all(down_half, "tensor", 0, 0, tiled=True)
    down_partner = lax.ppermute(down_own, "dp", [(i, i ^ 1) for i in range(lax.axis_size("dp"))])

    hidden, kept = up_stage(at, arrivals, norm_gain[None], weights)
    arrivals = gathered(at, hidden.reshape(count, hidden_dev))
    vocab_shape = pltpu.VMEM(vocab_w.shape, BF16)
    vocab_held = held(hold_vocab_kernel, vocab_shape, (arrivals[0][0][2],), (at, vocab_w))
    spots, pieces = split(sum(arrivals, ()))
    inputs = (at, *pieces, down_own, down_partner, kept.reshape(count, slice_w), digits)
    summed = pltpu.VMEM((count + EXTRA, slice_w), BF16)
    kernel = functools.partial(down_kernel, spots=spots)
    summed = call(kernel, summed, inputs, 2 * count * width * hidden_dev)
    arrivals = gathered(at, summed)
    stats = vocab_stage(at, arrivals, final_gain.reshape(PEERS, 1, slice_w), vocab_held, count)

    stats = jnp.moveaxis(stats[:3].reshape(3, PEERS, tok_local), 1, 0)
    stats = lax.all_to_all(stats, "tensor", 0, 0, tiled=True)
    largest = jnp.max(stats[:, 0], axis=0)
    total = jnp.sum(stats[:, 1] * jnp.exp(stats[:, 0] - largest), axis=0)
    own_losses = largest + jnp.log(total) - jnp.sum(stats[:, 2], axis=0)
    positions = mine * tok_local + lax.broadcasted_iota(jnp.int32, (tok_local,), 0)
    pack_ids = positions // PACK_LEN
    matches = pack_ids[:, None] == lax.broadcasted_iota(jnp.int32, (1, lengths.shape[0]), 1)
    limits = jnp.sum(jnp.where(matches, lengths[None, :], 0), axis=1)
    return jnp.where(positions % PACK_LEN < limits, own_losses, jnp.float32(0.0))


def solution(mesh):
    return jax.shard_map(
        body,
        mesh=mesh,
        in_specs=(
            P(("dp", "tensor"), None),
            P(),
            P(None, "tensor"),
            P(None, "tensor"),
            P("tensor", None),
            P(),
            P("tensor", None),
            P(("dp", "tensor")),
            P("dp"),
        ),
        out_specs=P(("dp", "tensor")),
        check_vma=False,
    )
```

```python
import functools

import jax
import jax.numpy as jnp
from jax import lax
from jax.experimental import pallas as pl
from jax.experimental.pallas import tpu as pltpu
from jax.sharding import PartitionSpec as P


PACK_LEN = 128
SIDE = 4
PEERS = SIDE * SIDE
OFFSETS = (0, SIDE - 1, 1, 2)
EXTRA = 16
EPS = 1e-06
BF16, F32 = jnp.bfloat16, jnp.float32
VMEM = pl.BlockSpec(memory_space=pltpu.VMEM)
SMEM = pl.BlockSpec(memory_space=pltpu.SMEM)
ANY = pl.BlockSpec(memory_space=pl.ANY)


def shifted(values, turn, step):
    pairs = []
    for part in range(lax.axis_size("dp")):
        for y in range(SIDE):
            for x in range(SIDE):
                along_x = (part % 2 == 0) == (turn == 0)
                to = (y, (x + step) % SIDE) if along_x else ((y + step) % SIDE, x)
                pairs.append((part * PEERS + y * SIDE + x, part * PEERS + to[0] * SIDE + to[1]))
    return lax.ppermute(values, ("dp", "tensor"), pairs)


def fanned(values):
    ways = (1, -1, 2)
    return [values, *(shifted(values, 0, step) for step in ways)]


def spot_of(at, group, block):
    ends = []
    for base, offset in ((at[0], group), (at[1], block)):
        ends.append(lax.rem(base + OFFSETS[offset], SIDE))
    return ends[0] * at[2] + ends[1] * at[3]


def call(kernel, out_shape, inputs, flops, scratch=()):
    inputs = inputs[:1] + tuple(pltpu.with_memory_space_constraint(a, pltpu.VMEM) for a in inputs[1:])
    return pl.pallas_call(
        kernel,
        compiler_params=pltpu.CompilerParams(vmem_limit_bytes=12 << 20),
        out_shape=out_shape,
        in_specs=[SMEM] + [VMEM] * (len(inputs) - 1),
        out_specs=jax.tree.map(lambda _: VMEM, out_shape),
        scratch_shapes=list(scratch),
        cost_estimate=pl.CostEstimate(flops=flops, transcendentals=0, bytes_accessed=1 << 20),
    )(*inputs)


def stack_kernel(at, *refs):
    blocks, (low, high) = refs[:SIDE], refs[-2:]
    rows, chunk = blocks[0].shape[0], 16

    def copy(step, carry):
        here = pl.ds(pl.multiple_of(step * chunk, chunk), chunk)
        for block in range(SIDE):
            (low, high)[block // 2][block % 2, here] = blocks[block][here]
        return carry

    lax.fori_loop(0, rows // chunk, copy, 0)


def gathered(at, values, own=None):
    half = pltpu.VMEM((2, *values.shape), values.dtype)
    own, arrived = values if own is None else own, fanned(values)[1:]
    low, high = call(stack_kernel, (half, half), (at, own, *arrived), 1 << 16)
    lower_low, upper_high = shifted(low, 1, 1), shifted(high, 1, -1)
    lower_high, upper_low = shifted(high, 1, 1), shifted(low, 1, -1)
    far_low, far_high = shifted(lower_low, 1, 1), shifted(upper_high, 1, -1)
    return (
        ((0, 0, low), (0, 2, high)),
        ((1, 0, lower_low), (2, 2, upper_high), (1, 2, lower_high), (2, 0, upper_low)),
        ((3, 0, far_low), (3, 2, far_high)),
    )


def hold_kernel(at, after, source, out):
    pltpu.sync_copy(source, out)


def prepare_kernel(at, targets, lengths, tokens, gate_w, up_w, down_w, *refs):
    out_tokens, out_up, out_down, digits, valid, sems = refs
    width, (peers, rows, slice_w) = gate_w.shape[1], out_down.shape
    pairs = [(tokens, out_tokens), (gate_w, out_up.at[:, :width]), (up_w, out_up.at[:, width:])]
    here = pl.ds(pl.multiple_of(at[4] * rows, rows), rows)
    for peer in range(peers):
        pairs.append((down_w.at[here, peer * slice_w : (peer + 1) * slice_w], out_down.at[peer]))
    copies = [pltpu.make_async_copy(source, to, sems.at[i]) for i, (source, to) in enumerate(pairs)]
    for copy in copies:
        copy.start()
    own, (extra, width) = targets.shape[0], digits.shape
    count = own * PEERS
    places = lax.broadcasted_iota(jnp.int32, (1, count), 1) - at[5] * own
    found = jnp.zeros((1, count), jnp.int32)
    for token in range(own):
        found = jnp.where(places == token, targets[token], found)
    block, row = jnp.zeros((extra, width), jnp.int32), lax.broadcasted_iota(jnp.int32, (extra, width), 0)
    for number, digit in enumerate((found // 256, found % 256)):
        for begin in range(0, count, width):
            block = jnp.where(row == (number * count + begin) // width, digit[:, begin : begin + width], block)
    digits[...] = block.astype(F32).astype(BF16)
    begin = at[5] * own
    places = lax.rem(begin, PACK_LEN) + lax.broadcasted_iota(jnp.int32, valid.shape, 1)
    valid[...] = (places < lengths[begin // PACK_LEN]).astype(F32)
    for copy in copies:
        copy.wait()


def held(kernel, out_shape, scalars, after, sources, scratch=()):
    after = tuple(pltpu.with_memory_space_constraint(a, pltpu.VMEM) for a in after)
    return pl.pallas_call(
        kernel,
        compiler_params=pltpu.CompilerParams(vmem_limit_bytes=2 << 20),
        out_shape=out_shape,
        in_specs=[SMEM] * len(scalars) + [VMEM] * len(after) + [ANY] * len(sources),
        out_specs=jax.tree.map(lambda _: VMEM, out_shape),
        scratch_shapes=list(scratch),
        cost_estimate=pl.CostEstimate(flops=1 << 31, transcendentals=0, bytes_accessed=16 << 20),
    )(*scalars, *after, *(pltpu.with_memory_space_constraint(a, pltpu.HBM) for a in sources))


def up_part(at, *refs, spots, earlier):
    count, last = len(spots), len(earlier) > 0
    pieces, (gain, weights), refs = refs[:count], refs[count : count + 2], refs[count + 2 :]
    sums, refs = refs[-1], refs[:-1]
    parts, ends = [], []
    if last:
        before = 2 * len(earlier)
        parts = [refs[i : i + 2] for i in range(0, before, 2)]
        ends, refs = refs[before : before + 2], refs[before + 2 :]
    hidden, kept = refs
    blocks, rows, width = pieces[0].shape
    tokens, step = blocks * rows, 512
    square = None
    for k in range(0, width, step):
        values = [ref[:, :, k : k + step].reshape(tokens, step) for ref in pieces]
        values = jnp.concatenate(values, axis=0).astype(F32)
        wide = values * values
        for c in range(0, step, 128):
            part = wide[:, c : c + 128]
            square = part if square is None else square + part
        scaled = (values * gain[:, k : k + step]).astype(BF16)
        product = jnp.dot(scaled, weights[k : k + step], preferred_element_type=F32)
        if k == 0:
            sums[...] = product
        else:
            sums[...] += product
    both = sums[...] * lax.rsqrt(jnp.sum(square, axis=1, keepdims=True) / width + EPS)
    gate, up = both[:, : both.shape[1] // 2], both[:, both.shape[1] // 2 :]
    result = (gate / (1.0 + jnp.exp(-gate)) * up).astype(BF16)
    hidden[...] = result.reshape(hidden.shape)
    slice_w = width // PEERS
    here = pl.ds(pl.multiple_of(at[5] * slice_w, slice_w), slice_w)
    for number in range(count):
        kept[number] = pieces[number][:, :, here]
    if not last:
        return
    for places, part in zip((*earlier, spots), (*parts, (hidden, kept))):
        for number, (group, block) in enumerate(places):
            for b in range(blocks):
                spot = spot_of(at, group, block + b)
                for end, ref in zip(ends, part):
                    end[spot] = ref[number, b]


def down_kernel(at, *refs, spots):
    pieces, (own, partner, kept, digits, out) = refs[: len(spots)], refs[len(spots) :]
    low = at[4] == 0
    count = kept.shape[0]
    total = kept[...].astype(F32)
    for piece, (group, block) in zip(pieces, spots):
        rhs = []
        for b in range(2):
            spot = spot_of(at, group, block + b)
            rhs.append(jnp.where(low, own[spot], partner[spot]))
            rhs.append(jnp.where(low, partner[spot], own[spot]))
        lhs = jnp.concatenate([piece[0], piece[1]], axis=1)
        total += jnp.dot(lhs, jnp.concatenate(rhs, axis=0), preferred_element_type=F32)
    out[:count] = total.astype(BF16)
    out[count:] = digits[...]


def vocab_part(at, *refs, spots, begin, last):
    pieces, (gain, vocab_w), refs = refs[: len(spots)], refs[len(spots) : len(spots) + 2], refs[len(spots) + 2 :]
    before, refs = (None, refs) if begin else (refs[:3], refs[3:])
    out, refs = (refs[0], refs[1:]) if last else (None, refs)
    logits, squares, digits = refs
    slice_w, count = gain.shape[2], logits.shape[1]
    square, digit = None, None
    for number, piece in enumerate(pieces):
        for block in range(2):
            spot = spot_of(at, spots[number][0], spots[number][1] + block)
            values = piece[block, :count].astype(F32)
            wide = values * values
            wide = wide[:, :128] + wide[:, 128:]
            square = wide if square is None else square + wide
            extra = piece[block, count:].astype(F32)
            digit = extra if digit is None else digit + extra
            scaled = (values * gain[spot]).astype(BF16)
            term = lax.dot_general(
                vocab_w[:, pl.ds(pl.multiple_of(spot * slice_w, slice_w), slice_w)],
                scaled,
                (((1,), (1,)), ((), ())),
                preferred_element_type=F32,
            )
            if number == 0 and block == 0:
                logits[...] = term if begin else before[0][...] + term
            else:
                logits[...] += term
    if not begin:
        square, digit = square + before[1][...], digit + before[2][...]
    squares[...], digits[...] = square, digit
    if last:
        vocab, width = vocab_w.shape
        total = jnp.sum(square.T, axis=0, keepdims=True)
        values = logits[...] * lax.rsqrt(total / width + EPS)
        largest = jnp.max(values, axis=0, keepdims=True)
        exponentials = jnp.sum(jnp.exp(values - largest), axis=0, keepdims=True)
        parts = count // slice_w
        high, low = (
            jnp.concatenate([digit[i * parts + p : i * parts + p + 1] for p in range(parts)], axis=1)
            for i in range(2)
        )
        wanted = (high * 256.0 + low).astype(jnp.int32) - at[5] * vocab
        found = lax.broadcasted_iota(jnp.int32, values.shape, 0) == wanted
        target = jnp.sum(jnp.where(found, values, 0.0), axis=0, keepdims=True)
        own = count // PEERS
        for peer in range(PEERS):
            for row, numbers in enumerate((largest, exponentials, target)):
                out[peer, row : row + 1] = numbers[:, peer * own : (peer + 1) * own]


def split(pieces):
    return tuple(piece[:2] for piece in pieces), tuple(piece[2] for piece in pieces)


def up_stage(at, arrivals, gain, weights):
    blocks, rows, width = arrivals[0][0][2].shape
    both, slice_w = weights.shape[1], width // PEERS
    earlier, before = (), ()
    for arrived in arrivals:
        spots, pieces = split(arrived)
        n, last = len(pieces), arrived is arrivals[-1]
        part_shape = tuple(pltpu.VMEM((n, blocks, rows, w), BF16) for w in (both // 2, slice_w))
        end_shape = tuple(pltpu.VMEM((PEERS, rows, w), BF16) for w in (both // 2, slice_w))
        sums = pltpu.VMEM((n * blocks * rows, both), F32)
        inputs = (at, *pieces, gain, weights)
        flops = 2 * n * blocks * rows * width * both
        if last:
            kernel = functools.partial(up_part, spots=spots, earlier=earlier)
            return call(kernel, end_shape, inputs + before, flops, (*part_shape, sums))
        kernel = functools.partial(up_part, spots=spots, earlier=())
        before += tuple(call(kernel, part_shape, inputs, flops, (sums,)))
        earlier += (spots,)


def vocab_stage(at, arrivals, gain, vocab_w, count):
    vocab, width = vocab_w.shape
    slice_w = width // PEERS
    sums = (
        pltpu.VMEM((vocab, count), F32),
        pltpu.VMEM((count, 128), F32),
        pltpu.VMEM((EXTRA, slice_w), F32),
    )
    results = ()
    for arrived in arrivals:
        spots, pieces = split(arrived)
        begin, last = arrived is arrivals[0], arrived is arrivals[-1]
        inputs = (at, *pieces, gain, vocab_w, *results)
        kernel = functools.partial(vocab_part, spots=spots, begin=begin, last=last)
        flops = 4 * count * width * vocab * len(pieces) // PEERS
        if last:
            return call(kernel, pltpu.VMEM((PEERS, 3, count // PEERS), F32), inputs, flops, sums)
        results = call(kernel, sums, inputs, flops)


def body(tokens, norm_gain, gate_w, up_w, down_w, final_gain, vocab_w, targets, lengths):
    tok_local, width = tokens.shape
    count = PEERS * tok_local
    hidden_dev, slice_w = gate_w.shape[1], width // PEERS
    mine = lax.axis_index("tensor")
    core = lax.rem(lax.axis_index("dp"), 2)
    y, x = mine // SIDE, lax.rem(mine, SIDE)
    even = core == 0
    at = [jnp.where(even, y, x), jnp.where(even, x, y), jnp.where(even, SIDE, 1), jnp.where(even, 1, SIDE)]
    at = jnp.stack(at + [core, mine]).astype(jnp.int32)

    shapes = (tokens.shape, (width, 2 * hidden_dev), (PEERS, hidden_dev // 2, slice_w), (EXTRA, slice_w))
    shapes = (*(pltpu.VMEM(shape, BF16) for shape in shapes), pltpu.VMEM((1, tok_local), F32))
    sems = pltpu.SemaphoreType.DMA((3 + PEERS,))
    sources = (tokens, gate_w, up_w, down_w)
    scalars = (at, targets, lengths)
    own, weights, down_half, digits, valid = held(prepare_kernel, shapes, scalars, (), sources, (sems,))
    arrivals = gathered(at, tokens, own)
    hidden, kept = up_stage(at, arrivals, norm_gain[None], weights)
    hidden = hidden.reshape(count, hidden_dev)
    arrivals = gathered(at, hidden)

    down_own = lax.all_to_all(down_half, "tensor", 0, 0, tiled=True)
    down_partner = lax.ppermute(down_own, "dp", [(i, i ^ 1) for i in range(lax.axis_size("dp"))])
    spots, pieces = split(sum(arrivals, ()))
    inputs = (at, *pieces, down_own, down_partner, kept.reshape(count, slice_w), digits)
    summed = pltpu.VMEM((count + EXTRA, slice_w), BF16)
    kernel = functools.partial(down_kernel, spots=spots)
    summed = call(kernel, summed, inputs, 2 * count * width * hidden_dev)
    vocab_held = held(hold_kernel, pltpu.VMEM(vocab_w.shape, BF16), (at,), (summed,), (vocab_w,))
    arrivals = gathered(at, summed)
    stats = vocab_stage(at, arrivals, final_gain.reshape(PEERS, 1, slice_w), vocab_held, count)

    stats = lax.all_to_all(stats, "tensor", 0, 0, tiled=True)
    largest = jnp.max(stats[:, 0], axis=0)
    total = jnp.sum(stats[:, 1] * jnp.exp(stats[:, 0] - largest), axis=0)
    own_losses = largest + jnp.log(total) - jnp.sum(stats[:, 2], axis=0)
    return jnp.where(valid[0] > 0.0, own_losses, 0.0)


def solution(mesh):
    return jax.shard_map(
        body,
        mesh=mesh,
        in_specs=(
            P(("dp", "tensor"), None),
            P(),
            P(None, "tensor"),
            P(None, "tensor"),
            P("tensor", None),
            P(),
            P("tensor", None),
            P(("dp", "tensor")),
            P("dp"),
        ),
        out_specs=P(("dp", "tensor")),
        check_vma=False,
    )
```
